512 devices in a mesh: seq: 256 (over y, z, x), head: 2 (over core).
Axes of the slice: x: 4, y: 8, z: 8, core: 2. Of those that a mesh axis runs over, the one named last changes fastest.
Arguments:
- hidden: bfloat16 [32768, 1024], P('seq'), may hold values from -24 to 24
- query_weight: bfloat16 [1024, 512], P(None, 'head'), may hold values from -0.1875 to 0.1875
- key_weight: bfloat16 [1024, 512], P(None, 'head'), may hold values from -0.1875 to 0.1875
- values: bfloat16 [32768, 512], P('seq', 'head'), may hold values from -6 to 6
- grad_out: bfloat16 [32768, 512], P('seq', 'head'), may hold values from -6 to 6
- random_feats: float32 [8, 64, 256], P('head'), may hold values from -4 to 4
Outputs:
- grad_hidden: float32 [32768, 1024], P('seq')
- grad_values: bfloat16 [32768, 512], P('seq', 'head')
- grad_query_weight: float32 [1024, 512], P('seq', 'head')
- grad_key_weight: float32 [1024, 512], P('seq', 'head')
The draws below stay inside these ranges and needn't reach their ends.
All inputs are finite; a program needn't handle non-finite values.
Results may differ from the reference program's by a relative error of at most 0.0038.
Values sent between devices are 32-bit elements; how exact they have to be, the bound alone decides.
A program may use at most 64 MiB of HBM per device.

```python
import jax
import jax.numpy as jnp
from jax import lax

D = 1024
HEADS = 8
DH = 64
M = 256
E = 512
S = 32768


def raised(drawn, own_key, source, target, blocks, factor):
    owner, partner = [(jnp.arange(drawn.shape[dim]) // (drawn.shape[dim] // blocks)).reshape([-1 if axis == dim else 1 for axis in range(drawn.ndim)]) for dim in (source, target)]
    chosen = jax.random.permutation(own_key, blocks)[partner]
    strong = (owner == chosen) | (owner == (partner + blocks // 2) % blocks)
    return jnp.where(strong, factor * drawn, drawn)


def steps_of(key, dims, split, least, top_value):
    def one(position, blocks):
        steps = jax.random.uniform(jax.random.fold_in(jax.random.fold_in(key, 6), position), (blocks,), jnp.float32, least / len(split), top_value / len(split))
        return jnp.repeat(jnp.exp(steps), dims[position] // blocks).reshape((-1,) + (1,) * (len(dims) - position - 1))

    gain = one(*split[0])
    for cut in split[1:]:
        gain = gain * one(*cut)
    return gain


def normal_values(own_key, extent, spread, reach, cuts=(), kind=jnp.bfloat16):
    result = jax.random.normal(own_key, extent, jnp.float32) * spread
    if len(cuts) > 0:
        result = steps_of(own_key, extent, cuts, -0.22, 0.18) * result
    return jnp.clip(result, min=-reach, max=reach).astype(kind)


def noise_with(key, dims, deviation, limit, split, heavy, dtype=jnp.bfloat16):
    entries = deviation * jax.random.normal(key, dims, jnp.float32)
    if split:
        entries = entries * steps_of(key, dims, split, -0.22, 0.18)
    return jnp.clip(raised(entries, jax.random.fold_in(key, 3), *heavy), -limit, limit).astype(dtype)


def setup_inputs(seed: int = 0) -> dict:
    key_of = jax.random.split(jax.random.key(seed), 7)
    return {
        "hidden": noise_with(key_of[0], (S, D), 1.0, 24.0, ((0, 256),), (0, 1, 256, 6.0)),
        "query_weight": normal_values(key_of[1], (D, E), D ** -0.5, 0.1875, ((1, 2),)),
        "key_weight": normal_values(key_of[2], (D, E), D ** -0.5, 0.1875, ((1, 2),)),
        "values": normal_values(key_of[3], (S, E), 1.0, 6.0, ((0, 256), (1, 2))),
        "grad_out": normal_values(key_of[4], (S, E), 1.0, 6.0, ((0, 256), (1, 2))),
        "random_feats": normal_values(key_of[5], (HEADS, DH, M), 1.0, 4.0, ((0, 2),), jnp.float32),
    }


HIGH = lax.Precision.HIGHEST

def features(rows, table):
    logits = jnp.dot(rows, table, precision=HIGH)
    half_norm = 0.5 * lax.optimization_barrier(jnp.sum(rows * rows, axis=1, keepdims=True))
    return jnp.exp(logits - half_norm) * M ** (-0.5)

def feature_grad(rows, feats, grads, table, feature_scale):
    weighted = feats * grads
    back = jnp.dot(weighted, table.T, precision=HIGH)
    return (back - rows * lax.optimization_barrier(jnp.sum(weighted, axis=1, keepdims=True))) * feature_scale

def one_head(packed):
    query_rows, key_rows, value_rows, upstream, table = packed
    feature_scale = DH ** (-0.25)
    query_feats = features(query_rows, table)
    key_feats = features(key_rows, table)
    value_state = jnp.dot(value_rows.T, key_feats, precision=HIGH)
    normalizer = lax.optimization_barrier(jnp.sum(key_feats, axis=0))
    numerator = jnp.dot(query_feats, value_state.T, precision=HIGH)
    denominator = jnp.dot(query_feats, normalizer, precision=HIGH)
    attended = numerator / denominator[:, None]
    grad_numer = upstream / denominator[:, None]
    grad_denom = -lax.optimization_barrier(jnp.sum(upstream * attended, axis=1)) / denominator
    grad_qfeat = jnp.dot(grad_numer, value_state, precision=HIGH) + grad_denom[:, None] * normalizer[None, :]
    grad_state = jnp.dot(grad_numer.T, query_feats, precision=HIGH)
    grad_normal = jnp.dot(grad_denom, query_feats, precision=HIGH)
    grad_kfeat = jnp.dot(value_rows, grad_state, precision=HIGH) + grad_normal[None, :]
    grad_value = jnp.dot(key_feats, grad_state.T, precision=HIGH)
    grad_query = feature_grad(query_rows, query_feats, grad_qfeat, table, feature_scale)
    grad_key = feature_grad(key_rows, key_feats, grad_kfeat, table, feature_scale)
    return (grad_query, grad_key, grad_value)

def split_heads(matrix):
    return matrix.reshape(S, HEADS, DH).transpose(1, 0, 2)

def join_heads(stacked):
    return stacked.transpose(1, 0, 2).reshape(S, E)

def reference(hidden, query_weight, key_weight, values, grad_out, random_feats):
    hidden_f = hidden.astype(jnp.float32)
    wq_f = query_weight.astype(jnp.float32)
    wk_f = key_weight.astype(jnp.float32)
    feature_scale = DH ** (-0.25)
    query_all = jnp.dot(hidden_f, wq_f, precision=HIGH) * feature_scale
    key_all = jnp.dot(hidden_f, wk_f, precision=HIGH) * feature_scale
    grad_query, grad_key, grad_value = lax.map(one_head, (split_heads(query_all), split_heads(key_all), split_heads(values.astype(jnp.float32)), split_heads(grad_out.astype(jnp.float32)), random_feats))
    dq_round = join_heads(grad_query).astype(jnp.bfloat16).astype(jnp.float32)
    dk_round = join_heads(grad_key).astype(jnp.bfloat16).astype(jnp.float32)
    grad_values = join_heads(grad_value).astype(jnp.bfloat16)
    grad_query_weight = jnp.dot(hidden_f.T, dq_round, precision=HIGH)
    grad_key_weight = jnp.dot(hidden_f.T, dk_round, precision=HIGH)
    grad_hidden = jnp.dot(dq_round, wq_f.T, precision=HIGH) + jnp.dot(dk_round, wk_f.T, precision=HIGH)
    return (grad_hidden, grad_values, grad_query_weight, grad_key_weight)
```

```python
import functools

import jax
import jax.numpy as jnp
from jax import lax
from jax.experimental import pallas as pl
from jax.experimental.pallas import tpu as pltpu
from jax.sharding import Mesh
from jax.sharding import PartitionSpec as P

F32 = jnp.float32
BF16 = jnp.bfloat16
Y, Z, X, H = "seq_0", "seq_1", "seq_2", "head"
SEQ = (Y, Z, X)
MESH = pl.DeviceIdType.MESH


def dg(a, b, ca, cb):
    return lax.dot_general(a, b, (((ca,), (cb,)), ((), ())), preferred_element_type=F32)


def split(a):
    hi = a.astype(BF16)
    return hi, (a - hi.astype(F32)).astype(BF16)


def dot2(a, b, ca=1, cb=0):
    hi, lo = split(b)
    return dg(a, hi, ca, cb) + dg(a, lo, ca, cb)


def dot3(a, b, ca=1, cb=0):
    ah, al = split(a)
    bh, bl = split(b)
    return dg(ah, bh, ca, cb) + (dg(ah, bl, ca, cb) + dg(al, bh, ca, cb))


class Exchange:
    def __init__(self, axis, count, recv, sems):
        self.axis, self.count, self.recv, self.sems = axis, count, recv, sems
        self.me = lax.axis_index(axis)

    def start(self, source, target=None):
        for d in range(1, self.count):
            other = lax.rem(self.me + d, self.count)
            pltpu.make_async_remote_copy(
                src_ref=source(other),
                dst_ref=self.recv.at[d - 1] if target is None else target,
                send_sem=self.sems.at[0],
                recv_sem=self.sems.at[1],
                device_id={self.axis: other},
                device_id_type=MESH,
            ).start()

    def wait(self):
        pltpu.make_async_copy(self.recv, self.recv, self.sems.at[1]).wait()

    def drain(self):
        pltpu.make_async_copy(self.recv, self.recv, self.sems.at[0]).wait()

    def total(self, own):
        for d in range(1, self.count):
            own = own + self.recv[d - 1]
        return own


class StateSum:
    def __init__(self, first, last, n, nx, state, r1, p1, r2, p2, r3, full, sems):
        self.state, self.p1, self.p2, self.full = state, p1, p2, full
        self.near = p1.shape[0]
        self.tile = p2.shape[0]
        self.steps = [
            Exchange(first, n, r1, sems.at[0]),
            Exchange(X, nx, r2, sems.at[1]),
            Exchange(last, n, r3, sems.at[2]),
            Exchange(X, nx, r2, sems.at[3]),
            Exchange(first, n, r1, sems.at[4]),
        ]
        self.base = pl.multiple_of(lax.axis_index(first) * self.near, self.near)
        self.x = lax.axis_index(X)

    def rows(self, start, count):
        return pl.ds(pl.multiple_of(start, 8), count)

    def start(self):
        self.steps[0].start(lambda j: self.state.at[self.rows(j * self.near, self.near)])

    def second(self):
        self.steps[0].wait()
        self.p1[...] = self.steps[0].total(self.state[self.rows(self.base, self.near)])
        self.steps[1].start(lambda j: self.p1.at[self.rows(j * self.tile, self.tile)])

    def third(self):
        self.steps[1].wait()
        self.p2[...] = self.steps[1].total(self.p1[self.rows(self.x * self.tile, self.tile)])
        self.steps[2].start(lambda j: self.p2)

    def fourth(self):
        self.steps[2].wait()
        spot = self.rows(self.base + self.x * self.tile, self.tile)
        self.full[spot] = self.steps[2].total(self.p2[...])
        self.steps[3].start(lambda j: self.full.at[spot], self.full.at[spot])

    def fifth(self):
        self.steps[3].wait()
        spot = self.rows(self.base, self.near)
        self.steps[4].start(lambda j: self.full.at[spot], self.full.at[spot])

    def finish(self):
        self.steps[4].wait()

    def drain(self):
        for step in self.steps:
            step.drain()


class RowSum:
    def __init__(self, order, counts, source, recvs, total, sems):
        self.source, self.result = source, total
        self.steps = [
            Exchange(axis, counts[axis], recvs[axis], sems.at[i]) for i, axis in enumerate(order)
        ]

    def start(self):
        self.steps[0].start(lambda j: self.source.at[0])

    def move(self, i):
        self.steps[i].wait()
        total = self.steps[i].total(self.source[i])
        if i == 2:
            self.result[...] = total
        else:
            self.source[i + 1] = total
            self.steps[i + 1].start(lambda j: self.source.at[i + 1])

    def drain(self):
        for step in self.steps:
            step.drain()


class WeightSum:
    def __init__(self, counts, tiles, rx, t1, ry, t2, rz, sems):
        self.tiles, self.t1, self.t2 = tiles, t1, t2
        self.x = Exchange(X, counts[X], rx, sems.at[0])
        self.y = Exchange(Y, counts[Y], ry, sems.at[1])
        self.z = Exchange(Z, counts[Z], rz, sems.at[2])

    def start(self):
        self.x.start(lambda j: self.tiles.at[j])

    def second(self):
        self.x.wait()
        self.t1[...] = self.x.total(self.tiles[self.x.me]).reshape(self.t1.shape)
        self.y.start(lambda j: self.t1.at[j])

    def third(self):
        self.y.wait()
        self.t2[...] = self.y.total(self.t1[self.y.me])
        self.z.start(lambda j: self.t2.at[j])

    def finish(self, out):
        self.z.wait()
        tile = self.z.total(self.t2[self.z.me])
        half = out.shape[0]
        out[:, 0:128] = tile[0:half]
        out[:, 128:256] = tile[half : 2 * half]

    def drain(self):
        for step in (self.x, self.y, self.z):
            step.drain()


def to_tiles(product, tiles):
    pairs = tiles.shape[0] // 2
    shape = (tiles.shape[1], pairs, 8, 128)
    left = product[:, 0:128].reshape(shape)
    right = product[:, 128:256].reshape(shape)
    upper = lax.broadcasted_iota(jnp.int32, (tiles.shape[1], 8, 128), 1) < 4
    for p in range(pairs):
        a, b = left[:, p], right[:, p]
        tiles[2 * p] = jnp.where(upper, a, pltpu.roll(b, 4, 1))
        tiles[2 * p + 1] = jnp.where(upper, pltpu.roll(a, 4, 1), b)


def kernel(counts, heads, dh, feat, hid, wq, wk, val, gout, tab, gh, gv, gq, gk, *scratch):
    (qs, ks, fa, fb, st, r1, p1, r2, p2, r3, full, st_sem) = scratch[:12]
    (zsrc, zy, zx, zz, ztot, z_sem) = scratch[12:18]
    (tiles, rx, t1, ry, t2, rz, w_sem) = scratch[18:25]
    (part, rpart, part_sem) = scratch[25:]
    ny, nz, nx = counts[Y], counts[Z], counts[X]
    scale = dh ** (-0.25)
    norm = feat ** (-0.5)

    barrier = pltpu.get_barrier_semaphore()
    partners = 0
    for axis, n in ((Y, ny), (Z, nz), (X, nx), (H, 2)):
        me = lax.axis_index(axis)
        for d in range(1, n):
            pl.semaphore_signal(
                barrier, inc=1, device_id={axis: lax.rem(me + d, n)}, device_id_type=MESH
            )
            partners += 1

    def state_sum(c):
        return [
            StateSum(
                (Y, Z)[i], (Z, Y)[i], ny, nx, st.at[c, i], r1.at[c, i], p1.at[c, i], r2.at[c, i],
                p2.at[c, i], r3.at[c, i], full.at[c, i], st_sem.at[c, i],
            )
            for i in range(2)
        ]

    def row_sum(c, order):
        recvs = {Y: zy.at[c], X: zx.at[c], Z: zz.at[c]}
        return RowSum(order, counts, zsrc.at[c], recvs, ztot.at[c], z_sem.at[c])

    def weight_sum(c):
        return WeightSum(
            counts, tiles.at[c], rx.at[c], t1.at[c], ry.at[c], t2.at[c], rz.at[c], w_sem.at[c]
        )

    usum, gsum = state_sum(0), state_sum(1)
    zsum, gzsum = row_sum(0, (Y, X, Z)), row_sum(1, (X, Y, Z))
    qsum, ksum = weight_sum(0), weight_sum(1)

    def cols(h):
        return slice(h * dh, (h + 1) * dh)

    def wide(h):
        return slice(h * feat, (h + 1) * feat)

    def features(rows, h):
        own = rows[:, cols(h)]
        logits = dot3(own, tab[h])
        half = 0.5 * jnp.sum(own * own, axis=1, keepdims=True)
        return jnp.exp(logits - half) * norm

    def put_state(c, h, block):
        st[c, 0, cols(h)] = block[:, 0:128]
        st[c, 1, cols(h)] = block[:, 128:256]

    def state(c, h):
        return jnp.concatenate([full[c, 0, cols(h)], full[c, 1, cols(h)]], axis=1)

    k = dg(hid[...], wk[...], 1, 0) * scale
    ks[...] = k
    vt = val[...].astype(F32).T.astype(BF16)
    for h in range(heads):
        b = features(k, h)
        fb[:, wide(h)] = b
        zsrc[0, 0, :, wide(h)] = jnp.sum(b, axis=0, keepdims=True)
        put_state(0, h, dot2(vt[cols(h)], b))
    pl.semaphore_wait(barrier, partners)
    zsum.start()
    for s in usum:
        s.start()

    q = dg(hid[...], wq[...], 1, 0) * scale
    qs[...] = q
    for h in range(heads):
        fa[:, wide(h)] = features(q, h)
    hid_t = hid[...].astype(F32).T.astype(BF16)
    zsum.move(0)
    for s in usum:
        s.second()
    zsum.move(1)
    for s in usum:
        s.third()
    zsum.move(2)

    g = gout[...].astype(F32)
    inv, gn = [], []
    for h in range(heads):
        a = fa[:, wide(h)]
        den = jnp.sum(a * ztot[0, :, wide(h)], axis=1, keepdims=True)
        inv.append(1.0 / den)
        gn.append(g[:, cols(h)] / den)
    gnt = jnp.concatenate(gn, axis=1).T
    for h in range(heads):
        put_state(1, h, dot3(gnt[cols(h)], fa[:, wide(h)]))
    for s in gsum:
        s.start()
    for s in usum:
        s.fourth()
    for s in usum:
        s.fifth()
    for s in gsum:
        s.second()
    for s in gsum:
        s.third()
    for s in usum:
        s.finish()

    gd = []
    for h in range(heads):
        a = fa[:, wide(h)]
        o = dot3(a, state(0, h), 1, 1) * inv[h]
        gd.append(-jnp.sum(g[:, cols(h)] * o, axis=1, keepdims=True) * inv[h])
        zsrc[1, 0, :, wide(h)] = jnp.sum(gd[h] * a, axis=0, keepdims=True)
    gzsum.start()
    for s in gsum:
        s.fourth()

    def back(rows, h, weighted):
        got = dot3(weighted, tab[h], 1, 1)
        total = jnp.sum(weighted, axis=1, keepdims=True)
        return ((got - rows[:, cols(h)] * total) * scale).astype(BF16)

    dq = []
    for h in range(heads):
        ga = dot3(gn[h], state(0, h)) + gd[h] * ztot[0, :, wide(h)]
        dq.append(back(qs, h, fa[:, wide(h)] * ga))
    dq = jnp.concatenate(dq, axis=1)
    gzsum.move(0)
    for s in gsum:
        s.fifth()
    to_tiles(dg(hid_t, dq, 1, 0), tiles.at[0])
    qsum.start()
    part[...] = dg(dq, wq[...], 1, 1)
    gzsum.move(1)
    for s in gsum:
        s.finish()
    for h in range(heads):
        gv[:, cols(h)] = dot3(fb[:, wide(h)], state(1, h), 1, 1).astype(BF16)
    gzsum.move(2)

    dk = []
    for h in range(heads):
        gb = dot2(val[:, cols(h)], state(1, h)) + ztot[1, :, wide(h)]
        dk.append(back(ks, h, fb[:, wide(h)] * gb))
    dk = jnp.concatenate(dk, axis=1)
    to_tiles(dg(hid_t, dk, 1, 0), tiles.at[1])
    ksum.start()
    part[...] += dg(dk, wk[...], 1, 1)
    swap = pltpu.make_async_remote_copy(
        src_ref=part,
        dst_ref=rpart,
        send_sem=part_sem.at[0],
        recv_sem=part_sem.at[1],
        device_id={H: 1 - lax.axis_index(H)},
        device_id_type=MESH,
    )
    swap.start()
    qsum.second()
    qsum.third()
    swap.wait_recv()
    gh[...] = part[...] + rpart[...]
    qsum.finish(gq)
    ksum.second()
    ksum.third()
    ksum.finish(gk)
    swap.wait_send()
    for s in usum + gsum + [zsum, gzsum, qsum, ksum]:
        s.drain()


def shards(counts, hidden, query_weight, key_weight, values, grad_out, random_feats):
    toks, depth = hidden.shape
    heads, dh, feat = random_feats.shape
    width = heads * dh
    ny, nz, nx = counts[Y], counts[Z], counts[X]
    near = width // ny
    tile = near // nx
    own_rows = depth // (ny * nz * nx)
    row = heads * feat
    vm = lambda *shape: pltpu.VMEM(shape, F32)
    dma = lambda *shape: pltpu.SemaphoreType.DMA(shape)
    scratch = [
        vm(toks, width),
        vm(toks, width),
        vm(toks, row),
        vm(toks, row),
        vm(2, 2, width, 128),
        vm(2, 2, ny - 1, near, 128),
        vm(2, 2, near, 128),
        vm(2, 2, nx - 1, tile, 128),
        vm(2, 2, tile, 128),
        vm(2, 2, nz - 1, tile, 128),
        vm(2, 2, width, 128),
        dma(2, 2, 5, 2),
        vm(2, 3, 1, row),
        vm(2, ny - 1, 1, row),
        vm(2, nx - 1, 1, row),
        vm(2, nz - 1, 1, row),
        vm(2, 1, row),
        dma(2, 3, 2),
        vm(2, nx, ny * nz, 8, 128),
        vm(2, nx - 1, ny * nz, 8, 128),
        vm(2, ny, nz, 8, 128),
        vm(2, ny - 1, nz, 8, 128),
        vm(2, nz, 8, 128),
        vm(2, nz - 1, 8, 128),
        dma(2, 3, 2),
        vm(toks, depth),
        vm(toks, depth),
        dma(2),
    ]
    return pl.pallas_call(
        functools.partial(kernel, counts, heads, dh, feat),
        out_shape=(
            jax.ShapeDtypeStruct((toks, depth), F32),
            jax.ShapeDtypeStruct((toks, width), BF16),
            jax.ShapeDtypeStruct((own_rows, width), F32),
            jax.ShapeDtypeStruct((own_rows, width), F32),
        ),
        in_specs=[pl.BlockSpec(memory_space=pltpu.VMEM)] * 6,
        out_specs=(pl.BlockSpec(memory_space=pltpu.VMEM),) * 4,
        scratch_shapes=scratch,
        compiler_params=pltpu.CompilerParams(collective_id=0, has_side_effects=True),
        name="favor_backward",
    )(hidden, query_weight, key_weight, values, grad_out, random_feats)


def build(torus):
    counts = {axis: torus.shape[axis] for axis in SEQ}
    return jax.shard_map(
        functools.partial(shards, counts),
        mesh=torus,
        in_specs=(
            P(SEQ, None),
            P(None, H),
            P(None, H),
            P(SEQ, H),
            P(SEQ, H),
            P(H, None, None),
        ),
        out_specs=(P(SEQ, None), P(SEQ, H), P(SEQ, H), P(SEQ, H)),
        check_vma=False,
    )


def solution(mesh):
    devices = mesh.devices.reshape(8, 8, 4, mesh.shape["head"])
    return build(Mesh(devices, (Y, Z, X, H)))
```

```python
import functools

import jax
import jax.numpy as jnp
from jax import lax
from jax.experimental import pallas as pl
from jax.experimental.pallas import tpu as pltpu
from jax.sharding import Mesh
from jax.sharding import PartitionSpec as P

F32 = jnp.float32
BF16 = jnp.bfloat16
Y, Z, X, H = "seq_0", "seq_1", "seq_2", "head"
SEQ = (Y, Z, X)
MESH = pl.DeviceIdType.MESH


def dg(a, b, ca, cb):
    return lax.dot_general(a, b, (((ca,), (cb,)), ((), ())), preferred_element_type=F32)


def split(a):
    hi = a.astype(BF16)
    return hi, (a - hi.astype(F32)).astype(BF16)


def dot2(a, b, ca=1, cb=0):
    hi, lo = split(b)
    return dg(a, hi, ca, cb) + dg(a, lo, ca, cb)


def dot3(a, b, ca=1, cb=0):
    ah, al = split(a)
    bh, bl = split(b)
    return dg(ah, bh, ca, cb) + (dg(ah, bl, ca, cb) + dg(al, bh, ca, cb))


class Exchange:
    def __init__(self, axis, count, recv, sems):
        self.axis, self.count, self.recv, self.sems = axis, count, recv, sems
        self.me = lax.axis_index(axis)

    def start(self, source, target=None):
        for d in range(1, self.count):
            other = lax.rem(self.me + d, self.count)
            pltpu.make_async_remote_copy(
                src_ref=source(other),
                dst_ref=self.recv.at[d - 1] if target is None else target,
                send_sem=self.sems.at[0],
                recv_sem=self.sems.at[1],
                device_id={self.axis: other},
                device_id_type=MESH,
            ).start()

    def wait(self):
        pltpu.make_async_copy(self.recv, self.recv, self.sems.at[1]).wait()

    def drain(self):
        pltpu.make_async_copy(self.recv, self.recv, self.sems.at[0]).wait()

    def total(self, own):
        for d in range(1, self.count):
            own = own + self.recv[d - 1]
        return own


class StateSum:
    def __init__(self, first, last, n, nx, state, r1, p1, r2, p2, r3, full, sems):
        self.state, self.p1, self.p2, self.full = state, p1, p2, full
        self.near = p1.shape[0]
        self.tile = p2.shape[0]
        self.steps = [
            Exchange(first, n, r1, sems.at[0]),
            Exchange(X, nx, r2, sems.at[1]),
            Exchange(last, n, r3, sems.at[2]),
            Exchange(X, nx, r2, sems.at[3]),
            Exchange(first, n, r1, sems.at[4]),
        ]
        self.base = pl.multiple_of(lax.axis_index(first) * self.near, self.near)
        self.x = lax.axis_index(X)

    def rows(self, start, count):
        return pl.ds(pl.multiple_of(start, 8), count)

    def start(self):
        self.steps[0].start(lambda j: self.state.at[self.rows(j * self.near, self.near)])

    def second(self):
        self.steps[0].wait()
        self.p1[...] = self.steps[0].total(self.state[self.rows(self.base, self.near)])
        self.steps[1].start(lambda j: self.p1.at[self.rows(j * self.tile, self.tile)])

    def third(self):
        self.steps[1].wait()
        self.p2[...] = self.steps[1].total(self.p1[self.rows(self.x * self.tile, self.tile)])
        self.steps[2].start(lambda j: self.p2)

    def fourth(self):
        self.steps[2].wait()
        spot = self.rows(self.base + self.x * self.tile, self.tile)
        self.full[spot] = self.steps[2].total(self.p2[...])
        self.steps[3].start(lambda j: self.full.at[spot], self.full.at[spot])

    def fifth(self):
        self.steps[3].wait()
        spot = self.rows(self.base, self.near)
        self.steps[4].start(lambda j: self.full.at[spot], self.full.at[spot])

    def finish(self):
        self.steps[4].wait()

    def drain(self):
        for step in self.steps:
            step.drain()


class RowSum:
    def __init__(self, order, counts, source, recvs, total, sems):
        self.source, self.result = source, total
        self.steps = [
            Exchange(axis, counts[axis], recvs[axis], sems.at[i]) for i, axis in enumerate(order)
        ]

    def start(self):
        self.steps[0].start(lambda j: self.source.at[0])

    def move(self, i):
        self.steps[i].wait()
        total = self.steps[i].total(self.source[i])
        if i == 2:
            self.result[...] = total
        else:
            self.source[i + 1] = total
            self.steps[i + 1].start(lambda j: self.source.at[i + 1])

    def drain(self):
        for step in self.steps:
            step.drain()


class WeightSum:
    def __init__(self, counts, hid_t, grads, rx, part, r1, p1, r2, sems):
        self.hid_t, self.grads, self.part, self.p1 = hid_t, grads, part, p1
        self.x = Exchange(X, counts[X], rx, sems.at[0])
        self.near = p1.shape[1]
        self.one = [
            Exchange(axis, counts[axis], r1.at[i], sems.at[1 + i]) for i, axis in enumerate((Y, Z))
        ]
        self.two = [
            Exchange(axis, counts[axis], r2.at[i], sems.at[3 + i]) for i, axis in enumerate((Z, Y))
        ]

    def start(self):
        self.x.start(lambda j: self.grads)

    def second(self):
        self.x.wait()
        for i in range(2):
            side = slice(i * 128, (i + 1) * 128)
            total = None
            for s in range(self.x.count):
                rows = self.grads[:, side] if s == 0 else self.x.recv[s - 1, :, side]
                term = dg(self.hid_t[i, s], rows.astype(BF16), 1, 0)
                total = term if total is None else total + term
            self.part[i] = total
            self.one[i].start(
                lambda j, i=i: self.part.at[i, pl.ds(pl.multiple_of(j * self.near, 8), self.near)]
            )

    def third(self):
        for i in range(2):
            one = self.one[i]
            one.wait()
            own = self.part[i, pl.ds(pl.multiple_of(one.me * self.near, 8), self.near)]
            self.p1[i] = one.total(own)
            self.two[i].start(
                lambda j, i=i: self.p1.at[i, pl.ds(pl.multiple_of(lax.div(j, 2) * 8, 8), 8)]
            )

    def finish(self, out):
        for i in range(2):
            two = self.two[i]
            two.wait()
            tile = two.total(self.p1[i, pl.ds(pl.multiple_of(lax.div(two.me, 2) * 8, 8), 8)])
            low = lax.rem(two.me, 2) == 0
            out[:, i * 128 : (i + 1) * 128] = jnp.where(low, tile[0:4], tile[4:8])

    def drain(self):
        for step in [self.x] + self.one + self.two:
            step.drain()


def interleave(upper, a, b):
    return jnp.where(upper, a, pltpu.roll(b, 4, 1)), jnp.where(upper, pltpu.roll(a, 4, 1), b)


def halves(shape):
    return lax.broadcasted_iota(jnp.int32, shape, 1) < 4


def by_x(turned, out):
    nx, rows, toks = out.shape
    tiles = turned.reshape(rows // 8, 2, nx // 2, 8, toks)
    upper = halves((rows // 8, 8, toks))
    for p in range(nx // 2):
        even, odd = interleave(upper, tiles[:, 0, p], tiles[:, 1, p])
        out[2 * p] = even.reshape(rows, toks)
        out[2 * p + 1] = odd.reshape(rows, toks)


def swapped(block, ny, nz):
    rows, toks = block.shape
    tiles = block.reshape(ny // 2, 2, nz // 2, 8, toks)
    upper = halves((ny // 2, 8, toks))
    out = []
    for w in range(nz // 2):
        out.extend(interleave(upper, tiles[:, 0, w], tiles[:, 1, w]))
    return jnp.concatenate([t.reshape(ny * 4, toks) for t in out], axis=0)


def kernel(counts, heads, dh, feat, hid, wq, wk, val, gout, tab, gh, gv, gq, gk, *scratch):
    (qs, ks, fa, fb, st, r1, p1, r2, p2, r3, full, st_sem) = scratch[:12]
    (zsrc, zy, zx, zz, ztot, z_sem) = scratch[12:18]
    (grads, rx, wpart, w1, wp1, w2, w_sem) = scratch[18:25]
    (turned, rturned, hid_t, turned_sem) = scratch[25:29]
    (part, rpart, part_sem) = scratch[29:]
    ny, nz, nx = counts[Y], counts[Z], counts[X]
    scale = dh ** (-0.25)
    norm = feat ** (-0.5)

    barrier = pltpu.get_barrier_semaphore()
    partners = 0
    for axis, n in ((Y, ny), (Z, nz), (X, nx), (H, 2)):
        me = lax.axis_index(axis)
        for d in range(1, n):
            pl.semaphore_signal(
                barrier, inc=1, device_id={axis: lax.rem(me + d, n)}, device_id_type=MESH
            )
            partners += 1

    def state_sum(c):
        return [
            StateSum(
                (Y, Z)[i], (Z, Y)[i], ny, nx, st.at[c, i], r1.at[c, i], p1.at[c, i], r2.at[c, i],
                p2.at[c, i], r3.at[c, i], full.at[c, i], st_sem.at[c, i],
            )
            for i in range(2)
        ]

    def row_sum(c, order):
        recvs = {Y: zy.at[c], X: zx.at[c], Z: zz.at[c]}
        return RowSum(order, counts, zsrc.at[c], recvs, ztot.at[c], z_sem.at[c])

    def weight_sum(c):
        return WeightSum(
            counts, hid_t, grads.at[c], rx.at[c], wpart.at[c], w1.at[c], wp1.at[c], w2.at[c], w_sem.at[c]
        )

    usum, gsum = state_sum(0), state_sum(1)
    zsum, gzsum = row_sum(0, (X, Y, Z)), row_sum(1, (X, Y, Z))
    qsum, ksum = weight_sum(0), weight_sum(1)
    hsum = Exchange(X, nx, rturned, turned_sem)

    def cols(h):
        return slice(h * dh, (h + 1) * dh)

    def wide(h):
        return slice(h * feat, (h + 1) * feat)

    def features(rows, h):
        own = rows[:, cols(h)]
        logits = dot3(own, tab[h])
        half = 0.5 * jnp.sum(own * own, axis=1, keepdims=True)
        return jnp.exp(logits - half) * norm

    def put_state(c, h, block):
        st[c, 0, cols(h)] = block[:, 0:128]
        st[c, 1, cols(h)] = block[:, 128:256]

    def state(c, h):
        return jnp.concatenate([full[c, 0, cols(h)], full[c, 1, cols(h)]], axis=1)

    k = dg(hid[...], wk[...], 1, 0) * scale
    ks[...] = k
    vt = val[...].astype(F32).T.astype(BF16)
    for h in range(heads):
        b = features(k, h)
        fb[:, wide(h)] = b
        zsrc[0, 0, :, wide(h)] = jnp.sum(b, axis=0, keepdims=True)
        put_state(0, h, dot2(vt[cols(h)], b))
    pl.semaphore_wait(barrier, partners)
    zsum.start()
    for s in usum:
        s.start()
    by_x(hid[...].astype(F32).T, turned)
    hsum.start(lambda j: turned.at[j])

    q = dg(hid[...], wq[...], 1, 0) * scale
    qs[...] = q
    for h in range(heads):
        fa[:, wide(h)] = features(q, h)
    zsum.move(0)
    for s in usum:
        s.second()
    zsum.move(1)
    for s in usum:
        s.third()
    zsum.move(2)

    g = gout[...].astype(F32)
    inv, gn = [], []
    for h in range(heads):
        a = fa[:, wide(h)]
        den = jnp.sum(a * ztot[0, :, wide(h)], axis=1, keepdims=True)
        inv.append(1.0 / den)
        gn.append(g[:, cols(h)] / den)
    gnt = jnp.concatenate(gn, axis=1).T
    for h in range(heads):
        put_state(1, h, dot3(gnt[cols(h)], fa[:, wide(h)]))
    for s in gsum:
        s.start()
    for s in usum:
        s.fourth()
    for s in usum:
        s.fifth()
    hsum.wait()
    for i in range(nx):
        block = turned[hsum.me] if i == 0 else rturned[i - 1]
        hid_t[0, i] = block.astype(BF16)
        hid_t[1, i] = swapped(block, ny, nz).astype(BF16)
    for s in gsum:
        s.second()
    for s in gsum:
        s.third()
    for s in usum:
        s.finish()

    gd = []
    for h in range(heads):
        a = fa[:, wide(h)]
        o = dot3(a, state(0, h), 1, 1) * inv[h]
        gd.append(-jnp.sum(g[:, cols(h)] * o, axis=1, keepdims=True) * inv[h])
        zsrc[1, 0, :, wide(h)] = jnp.sum(gd[h] * a, axis=0, keepdims=True)
    gzsum.start()
    for s in gsum:
        s.fourth()

    def back(rows, h, weighted):
        got = dot3(weighted, tab[h], 1, 1)
        total = jnp.sum(weighted, axis=1, keepdims=True)
        return ((got - rows[:, cols(h)] * total) * scale).astype(BF16)

    dq = []
    for h in range(heads):
        ga = dot3(gn[h], state(0, h)) + gd[h] * ztot[0, :, wide(h)]
        dq.append(back(qs, h, fa[:, wide(h)] * ga))
    dq = jnp.concatenate(dq, axis=1)
    gzsum.move(0)
    for s in gsum:
        s.fifth()
    grads[0] = dq.astype(F32)
    qsum.start()
    part[...] = dg(dq, wq[...], 1, 1)
    gzsum.move(1)
    for s in gsum:
        s.finish()
    qsum.second()
    for h in range(heads):
        gv[:, cols(h)] = dot3(fb[:, wide(h)], state(1, h), 1, 1).astype(BF16)
    gzsum.move(2)

    dk = []
    for h in range(heads):
        gb = dot2(val[:, cols(h)], state(1, h)) + ztot[1, :, wide(h)]
        dk.append(back(ks, h, fb[:, wide(h)] * gb))
    dk = jnp.concatenate(dk, axis=1)
    grads[1] = dk.astype(F32)
    ksum.start()
    part[...] += dg(dk, wk[...], 1, 1)
    swap = pltpu.make_async_remote_copy(
        src_ref=part,
        dst_ref=rpart,
        send_sem=part_sem.at[0],
        recv_sem=part_sem.at[1],
        device_id={H: 1 - lax.axis_index(H)},
        device_id_type=MESH,
    )
    swap.start()
    qsum.third()
    ksum.second()
    swap.wait_recv()
    gh[...] = part[...] + rpart[...]
    qsum.finish(gq)
    ksum.third()
    ksum.finish(gk)
    swap.wait_send()
    for s in usum + gsum + [zsum, gzsum, qsum, ksum, hsum]:
        s.drain()


def settle(*refs):
    for source, target in zip(refs[:4], refs[4:]):
        target[...] = source[...]


def shards(counts, hidden, query_weight, key_weight, values, grad_out, random_feats):
    toks, depth = hidden.shape
    heads, dh, feat = random_feats.shape
    width = heads * dh
    ny, nz, nx = counts[Y], counts[Z], counts[X]
    near = width // ny
    tile = near // nx
    own_rows = depth // (ny * nz * nx)
    row = heads * feat
    rows = depth // nx
    vm = lambda *shape: pltpu.VMEM(shape, F32)
    dma = lambda *shape: pltpu.SemaphoreType.DMA(shape)
    scratch = [
        vm(toks, width),
        vm(toks, width),
        vm(toks, row),
        vm(toks, row),
        vm(2, 2, width, 128),
        vm(2, 2, ny - 1, near, 128),
        vm(2, 2, near, 128),
        vm(2, 2, nx - 1, tile, 128),
        vm(2, 2, tile, 128),
        vm(2, 2, nz - 1, tile, 128),
        vm(2, 2, width, 128),
        dma(2, 2, 5, 2),
        vm(2, 3, 1, row),
        vm(2, ny - 1, 1, row),
        vm(2, nx - 1, 1, row),
        vm(2, nz - 1, 1, row),
        vm(2, 1, row),
        dma(2, 3, 2),
        vm(2, toks, width),
        vm(2, nx - 1, toks, width),
        vm(2, 2, rows, 128),
        vm(2, 2, ny - 1, rows // ny, 128),
        vm(2, 2, rows // ny, 128),
        vm(2, 2, nz - 1, 8, 128),
        dma(2, 5, 2),
        vm(nx, rows, toks),
        vm(nx - 1, rows, toks),
        pltpu.VMEM((2, nx, rows, toks), BF16),
        dma(2),
        vm(toks, depth),
        vm(toks, depth),
        dma(2),
    ]
    shapes = (
        jax.ShapeDtypeStruct((toks, depth), F32),
        jax.ShapeDtypeStruct((toks, width), BF16),
        jax.ShapeDtypeStruct((own_rows, width), F32),
        jax.ShapeDtypeStruct((own_rows, width), F32),
    )
    vmem = pl.BlockSpec(memory_space=pltpu.VMEM)
    results = pl.pallas_call(
        functools.partial(kernel, counts, heads, dh, feat),
        out_shape=shapes,
        in_specs=[vmem] * 6,
        out_specs=(vmem,) * 4,
        scratch_shapes=scratch,
        compiler_params=pltpu.CompilerParams(collective_id=0, has_side_effects=True),
        name="favor_backward",
    )(hidden, query_weight, key_weight, values, grad_out, random_feats)
    return pl.pallas_call(
        settle, out_shape=shapes, in_specs=[vmem] * 4, out_specs=(vmem,) * 4, name="settle"
    )(*results)


def build(torus):
    counts = {axis: torus.shape[axis] for axis in SEQ}
    return jax.shard_map(
        functools.partial(shards, counts),
        mesh=torus,
        in_specs=(
            P(SEQ, None),
            P(None, H),
            P(None, H),
            P(SEQ, H),
            P(SEQ, H),
            P(H, None, None),
        ),
        out_specs=(P(SEQ, None), P(SEQ, H), P(SEQ, H), P(SEQ, H)),
        check_vma=False,
    )


def solution(mesh):
    devices = mesh.devices.reshape(8, 8, 4, mesh.shape["head"])
    return build(Mesh(devices, (Y, Z, X, H)))
```

```python
import functools
import itertools

import jax
import jax.numpy as jnp
from jax import lax
from jax.experimental import pallas as pl
from jax.experimental.pallas import tpu as pltpu
from jax.sharding import Mesh
from jax.sharding import PartitionSpec as P

F32 = jnp.float32
BF16 = jnp.bfloat16
Y, Z, X, H = "seq_0", "seq_1", "seq_2", "head"
SEQ = (Y, Z, X)
MESH = pl.DeviceIdType.MESH


def dg(a, b, ca, cb):
    return lax.dot_general(a, b, (((ca,), (cb,)), ((), ())), preferred_element_type=F32)


def split(a):
    hi = a.astype(BF16)
    return hi, (a - hi.astype(F32)).astype(BF16)


def dot2(a, b, ca=1, cb=0):
    hi, lo = split(b)
    return dg(a, hi, ca, cb) + dg(a, lo, ca, cb)


def dot3(a, b, ca=1, cb=0):
    ah, al = split(a)
    bh, bl = split(b)
    return dg(ah, bh, ca, cb) + (dg(ah, bl, ca, cb) + dg(al, bh, ca, cb))


class Exchange:
    def __init__(self, axes, counts, recv, sems):
        self.axes, self.recv, self.sems = axes, recv, sems
        self.counts = [counts[axis] for axis in axes]
        self.me = [lax.axis_index(axis) for axis in axes]
        self.moves = other_moves(self.counts)

    def start(self, source, target=None):
        places = [
            [lax.rem(m + d, n) for d in range(n)] for m, n in zip(self.me, self.counts)
        ]
        for slot, move in enumerate(self.moves):
            other = [place[d] for place, d in zip(places, move)]
            pltpu.make_async_remote_copy(
                src_ref=source(*other),
                dst_ref=self.recv.at[slot] if target is None else target,
                send_sem=self.sems.at[0],
                recv_sem=self.sems.at[1],
                device_id=dict(zip(self.axes, other)),
                device_id_type=MESH,
            ).start()

    def wait(self):
        pltpu.make_async_copy(self.recv, self.recv, self.sems.at[1]).wait()

    def drain(self):
        pltpu.make_async_copy(self.recv, self.recv, self.sems.at[0]).wait()

    def total(self, own):
        parts = [own] + [self.recv[slot] for slot in range(len(self.moves))]
        while len(parts) > 1:
            odd = parts[len(parts) // 2 * 2 :]
            parts = [a + b for a, b in zip(parts[0::2], parts[1::2])] + odd
        return parts[0]


def other_moves(counts):
    def hops(move):
        return sum(min(d, n - d) for d, n in zip(move, counts))

    moves = [m for m in itertools.product(*(range(n) for n in counts)) if any(m)]
    return sorted(moves, key=hops, reverse=True)


class StateSum:
    def __init__(self, first, last, counts, state, r1, p1, r2, full, sems):
        self.state, self.p1, self.full = state, p1, full
        self.tile, self.nx = p1.shape[0], counts[X]
        self.scatter = Exchange((first, X), counts, r1, sems.at[0])
        self.line = Exchange((last,), counts, r2, sems.at[1])
        self.gather = Exchange((first, X), counts, r1, sems.at[2])

    def spot(self, first, x):
        return pl.ds(pl.multiple_of((first * self.nx + x) * self.tile, 8), self.tile)

    def start(self):
        self.scatter.start(lambda first, x: self.state.at[self.spot(first, x)])

    def second(self):
        self.scatter.wait()
        self.p1[...] = self.scatter.total(self.state[self.spot(*self.scatter.me)])
        self.line.start(lambda j: self.p1)

    def third(self):
        self.line.wait()
        own = self.spot(*self.scatter.me)
        self.full[own] = self.line.total(self.p1[...])
        self.gather.start(lambda first, x: self.full.at[own], self.full.at[own])

    def finish(self):
        self.gather.wait()

    def drain(self):
        for step in (self.scatter, self.line, self.gather):
            step.drain()


class RowSum:
    def __init__(self, counts, source, plane, line, result, sems):
        self.source, self.result = source, result
        self.plane = Exchange((Y, X), counts, plane, sems.at[0])
        self.line = Exchange((Z,), counts, line, sems.at[1])

    def start(self):
        self.plane.start(lambda *_: self.source.at[0])

    def second(self):
        self.plane.wait()
        self.source[1] = self.plane.total(self.source[0])
        self.line.start(lambda _: self.source.at[1])

    def finish(self):
        self.line.wait()
        self.result[...] = self.line.total(self.source[1])

    def drain(self):
        for step in (self.plane, self.line):
            step.drain()


class WeightSum:
    def __init__(self, counts, hid_t, grads, rx, part, r1, p1, r2, sems):
        self.hid_t, self.grads, self.part, self.p1 = hid_t, grads, part, p1
        self.x = Exchange((X,), counts, rx, sems.at[0])
        self.near = p1.shape[1]
        self.one = [
            Exchange((axis,), counts, r1.at[i], sems.at[1 + i]) for i, axis in enumerate((Y, Z))
        ]
        self.two = [
            Exchange((axis,), counts, r2.at[i], sems.at[3 + i]) for i, axis in enumerate((Z, Y))
        ]

    def start(self):
        self.x.start(lambda j: self.grads)

    def second(self):
        self.x.wait()
        for i in range(2):
            side = slice(i * 128, (i + 1) * 128)
            total = None
            for s in range(self.x.counts[0]):
                rows = self.grads[:, side] if s == 0 else self.x.recv[s - 1, :, side]
                term = dg(self.hid_t[i, s], rows.astype(BF16), 1, 0)
                total = term if total is None else total + term
            self.part[i] = total
            self.one[i].start(
                lambda j, i=i: self.part.at[i, pl.ds(pl.multiple_of(j * self.near, 8), self.near)]
            )

    def third(self):
        for i in range(2):
            one = self.one[i]
            one.wait()
            own = self.part[i, pl.ds(pl.multiple_of(one.me[0] * self.near, 8), self.near)]
            self.p1[i] = one.total(own)
            self.two[i].start(
                lambda j, i=i: self.p1.at[i, pl.ds(pl.multiple_of(lax.div(j, 2) * 8, 8), 8)]
            )

    def finish(self, out):
        for i in range(2):
            two = self.two[i]
            two.wait()
            tile = two.total(self.p1[i, pl.ds(pl.multiple_of(lax.div(two.me[0], 2) * 8, 8), 8)])
            low = lax.rem(two.me[0], 2) == 0
            out[:, i * 128 : (i + 1) * 128] = jnp.where(low, tile[0:4], tile[4:8])

    def drain(self):
        for step in [self.x] + self.one + self.two:
            step.drain()


def interleave(upper, a, b):
    return jnp.where(upper, a, pltpu.roll(b, 4, 1)), jnp.where(upper, pltpu.roll(a, 4, 1), b)


def halves(shape):
    return lax.broadcasted_iota(jnp.int32, shape, 1) < 4


def by_x(turned, out):
    nx, rows, toks = out.shape
    tiles = turned.reshape(rows // 8, 2, nx // 2, 8, toks)
    upper = halves((rows // 8, 8, toks))
    for p in range(nx // 2):
        even, odd = interleave(upper, tiles[:, 0, p], tiles[:, 1, p])
        out[2 * p] = even.reshape(rows, toks)
        out[2 * p + 1] = odd.reshape(rows, toks)


def swapped(block, ny, nz):
    rows, toks = block.shape
    tiles = block.reshape(ny // 2, 2, nz // 2, 8, toks)
    upper = halves((ny // 2, 8, toks))
    out = []
    for w in range(nz // 2):
        out.extend(interleave(upper, tiles[:, 0, w], tiles[:, 1, w]))
    return jnp.concatenate([t.reshape(ny * 4, toks) for t in out], axis=0)


def kernel(counts, heads, dh, feat, hid, wq, wk, val, gout, tab, gh, gv, gq, gk, *scratch):
    (qs, ks, fa, fb, st, r1, p1, r2, full, st_sem) = scratch[:10]
    (zsrc, zp, zl, ztot, z_sem) = scratch[10:15]
    (grads, rx, wpart, w1, wp1, w2, w_sem) = scratch[15:22]
    (turned, rturned, hid_t, turned_sem) = scratch[22:26]
    (part, rpart, part_sem) = scratch[26:]
    ny, nz, nx = counts[Y], counts[Z], counts[X]
    sizes = {**counts, H: 2}
    scale = dh ** (-0.25)
    norm = feat ** (-0.5)

    barrier = pltpu.get_barrier_semaphore()
    partners = set()
    for axes in ((Y, X), (Z, X), (H,)):
        for move in other_moves([sizes[axis] for axis in axes]):
            partners.add(tuple(sorted(zip(axes, move))))
    partners = sorted({tuple((a, d) for a, d in move if d) for move in partners})
    for move in partners:
        place = {a: lax.rem(lax.axis_index(a) + d, sizes[a]) for a, d in move}
        pl.semaphore_signal(barrier, inc=1, device_id=place, device_id_type=MESH)

    def state_sum(c):
        return [
            StateSum(
                (Y, Z)[i], (Z, Y)[i], counts, st.at[c, i], r1.at[c, i], p1.at[c, i], r2.at[c, i],
                full.at[c, i], st_sem.at[c, i],
            )
            for i in range(2)
        ]

    def row_sum(c):
        return RowSum(counts, zsrc.at[c], zp.at[c], zl.at[c], ztot.at[c], z_sem.at[c])

    def weight_sum(c):
        return WeightSum(
            counts, hid_t, grads.at[c], rx.at[c], wpart.at[c], w1.at[c], wp1.at[c], w2.at[c], w_sem.at[c]
        )

    usum, gsum = state_sum(0), state_sum(1)
    zsum, gzsum = row_sum(0), row_sum(1)
    qsum, ksum = weight_sum(0), weight_sum(1)
    hsum = Exchange((X,), counts, rturned, turned_sem)

    def cols(h):
        return slice(h * dh, (h + 1) * dh)

    def wide(h):
        return slice(h * feat, (h + 1) * feat)

    def features(rows, h):
        own = rows[:, cols(h)]
        logits = dot3(own, tab[h])
        half = 0.5 * jnp.sum(own * own, axis=1, keepdims=True)
        return jnp.exp(logits - half) * norm

    def put_state(c, h, block):
        st[c, 0, cols(h)] = block[:, 0:128]
        st[c, 1, cols(h)] = block[:, 128:256]

    def state(c, h):
        return jnp.concatenate([full[c, 0, cols(h)], full[c, 1, cols(h)]], axis=1)

    k = dg(hid[...], wk[...], 1, 0) * scale
    ks[...] = k
    vt = val[...].astype(F32).T.astype(BF16)
    for h in range(heads):
        b = features(k, h)
        fb[:, wide(h)] = b
        zsrc[0, 0, :, wide(h)] = jnp.sum(b, axis=0, keepdims=True)
        put_state(0, h, dot2(vt[cols(h)], b))
    pl.semaphore_wait(barrier, len(partners))
    zsum.start()
    for s in usum:
        s.start()
    by_x(hid[...].astype(F32).T, turned)
    hsum.start(lambda j: turned.at[j])

    q = dg(hid[...], wq[...], 1, 0) * scale
    qs[...] = q
    for h in range(heads):
        fa[:, wide(h)] = features(q, h)
    zsum.second()
    for s in usum:
        s.second()
    zsum.finish()

    g = gout[...].astype(F32)
    inv, gn = [], []
    for h in range(heads):
        a = fa[:, wide(h)]
        den = jnp.sum(a * ztot[0, :, wide(h)], axis=1, keepdims=True)
        inv.append(1.0 / den)
        gn.append(g[:, cols(h)] / den)
    gnt = jnp.concatenate(gn, axis=1).T
    for h in range(heads):
        put_state(1, h, dot3(gnt[cols(h)], fa[:, wide(h)]))
    for s in gsum:
        s.start()
    for s in usum:
        s.third()
    hsum.wait()
    for i in range(nx):
        block = turned[hsum.me[0]] if i == 0 else rturned[i - 1]
        hid_t[0, i] = block.astype(BF16)
        hid_t[1, i] = swapped(block, ny, nz).astype(BF16)
    for s in gsum:
        s.second()
    for s in usum:
        s.finish()

    gd = []
    for h in range(heads):
        a = fa[:, wide(h)]
        o = dot3(a, state(0, h), 1, 1) * inv[h]
        gd.append(-jnp.sum(g[:, cols(h)] * o, axis=1, keepdims=True) * inv[h])
        zsrc[1, 0, :, wide(h)] = jnp.sum(gd[h] * a, axis=0, keepdims=True)
    gzsum.start()
    for s in gsum:
        s.third()

    def back(rows, h, weighted):
        got = dot3(weighted, tab[h], 1, 1)
        total = jnp.sum(weighted, axis=1, keepdims=True)
        return ((got - rows[:, cols(h)] * total) * scale).astype(BF16)

    dq = []
    for h in range(heads):
        ga = dot3(gn[h], state(0, h)) + gd[h] * ztot[0, :, wide(h)]
        dq.append(back(qs, h, fa[:, wide(h)] * ga))
    dq = jnp.concatenate(dq, axis=1)
    gzsum.second()
    grads[0] = dq.astype(F32)
    qsum.start()
    part[...] = dg(dq, wq[...], 1, 1)
    for s in gsum:
        s.finish()
    for h in range(heads):
        gv[:, cols(h)] = dot3(fb[:, wide(h)], state(1, h), 1, 1).astype(BF16)
    gzsum.finish()

    dk = []
    for h in range(heads):
        gb = dot2(val[:, cols(h)], state(1, h)) + ztot[1, :, wide(h)]
        dk.append(back(ks, h, fb[:, wide(h)] * gb))
    dk = jnp.concatenate(dk, axis=1)
    grads[1] = dk.astype(F32)
    ksum.start()
    qsum.second()
    part[...] += dg(dk, wk[...], 1, 1)
    swap = pltpu.make_async_remote_copy(
        src_ref=part,
        dst_ref=rpart,
        send_sem=part_sem.at[0],
        recv_sem=part_sem.at[1],
        device_id={H: 1 - lax.axis_index(H)},
        device_id_type=MESH,
    )
    swap.start()
    qsum.third()
    ksum.second()
    swap.wait_recv()
    gh[...] = part[...] + rpart[...]
    qsum.finish(gq)
    ksum.third()
    ksum.finish(gk)
    swap.wait_send()
    for s in usum + gsum + [zsum, gzsum, qsum, ksum, hsum]:
        s.drain()


def settle(*refs):
    for source, target in zip(refs[:4], refs[4:]):
        target[...] = source[...]


def shards(counts, hidden, query_weight, key_weight, values, grad_out, random_feats):
    toks, depth = hidden.shape
    heads, dh, feat = random_feats.shape
    width = heads * dh
    ny, nz, nx = counts[Y], counts[Z], counts[X]
    tile = width // (ny * nx)
    own_rows = depth // (ny * nz * nx)
    row = heads * feat
    rows = depth // nx
    vm = lambda *shape: pltpu.VMEM(shape, F32)
    dma = lambda *shape: pltpu.SemaphoreType.DMA(shape)
    scratch = [
        vm(toks, width),
        vm(toks, width),
        vm(toks, row),
        vm(toks, row),
        vm(2, 2, width, 128),
        vm(2, 2, ny * nx - 1, tile, 128),
        vm(2, 2, tile, 128),
        vm(2, 2, nz - 1, tile, 128),
        vm(2, 2, width, 128),
        dma(2, 2, 3, 2),
        vm(2, 2, 1, row),
        vm(2, ny * nx - 1, 1, row),
        vm(2, nz - 1, 1, row),
        vm(2, 1, row),
        dma(2, 2, 2),
        vm(2, toks, width),
        vm(2, nx - 1, toks, width),
        vm(2, 2, rows, 128),
        vm(2, 2, ny - 1, rows // ny, 128),
        vm(2, 2, rows // ny, 128),
        vm(2, 2, nz - 1, 8, 128),
        dma(2, 5, 2),
        vm(nx, rows, toks),
        vm(nx - 1, rows, toks),
        pltpu.VMEM((2, nx, rows, toks), BF16),
        dma(2),
        vm(toks, depth),
        vm(toks, depth),
        dma(2),
    ]
    shapes = (
        jax.ShapeDtypeStruct((toks, depth), F32),
        jax.ShapeDtypeStruct((toks, width), BF16),
        jax.ShapeDtypeStruct((own_rows, width), F32),
        jax.ShapeDtypeStruct((own_rows, width), F32),
    )
    vmem = pl.BlockSpec(memory_space=pltpu.VMEM)
    results = pl.pallas_call(
        functools.partial(kernel, counts, heads, dh, feat),
        out_shape=shapes,
        in_specs=[vmem] * 6,
        out_specs=(vmem,) * 4,
        scratch_shapes=scratch,
        compiler_params=pltpu.CompilerParams(collective_id=0, has_side_effects=True),
        name="favor_backward",
    )(hidden, query_weight, key_weight, values, grad_out, random_feats)
    return pl.pallas_call(
        settle, out_shape=shapes, in_specs=[vmem] * 4, out_specs=(vmem,) * 4, name="settle"
    )(*results)


def build(torus):
    counts = {axis: torus.shape[axis] for axis in SEQ}
    return jax.shard_map(
        functools.partial(shards, counts),
        mesh=torus,
        in_specs=(
            P(SEQ, None),
            P(None, H),
            P(None, H),
            P(SEQ, H),
            P(SEQ, H),
            P(H, None, None),
        ),
        out_specs=(P(SEQ, None), P(SEQ, H), P(SEQ, H), P(SEQ, H)),
        check_vma=False,
    )


def solution(mesh):
    devices = mesh.devices.reshape(8, 8, 4, mesh.shape["head"])
    return build(Mesh(devices, (Y, Z, X, H)))
```

```python
import functools
import itertools

import jax
import jax.numpy as jnp
from jax import lax
from jax.experimental import pallas as pl
from jax.experimental.pallas import tpu as pltpu
from jax.sharding import Mesh
from jax.sharding import PartitionSpec as P

F32 = jnp.float32
BF16 = jnp.bfloat16
Y, Z, X, H = "seq_0", "seq_1", "seq_2", "head"
SEQ = (Y, Z, X)
MESH = pl.DeviceIdType.MESH


def dg(a, b, ca, cb):
    return lax.dot_general(a, b, (((ca,), (cb,)), ((), ())), preferred_element_type=F32)


def split(a):
    hi = a.astype(BF16)
    return hi, (a - hi.astype(F32)).astype(BF16)


def dot2(a, b, ca=1, cb=0):
    hi, lo = split(b)
    return dg(a, hi, ca, cb) + dg(a, lo, ca, cb)


def dot3(a, b, ca=1, cb=0):
    ah, al = split(a)
    bh, bl = split(b)
    return dg(ah, bh, ca, cb) + (dg(ah, bl, ca, cb) + dg(al, bh, ca, cb))


class Exchange:
    def __init__(self, axes, counts, recv, sems):
        self.axes, self.recv, self.sems = axes, recv, sems
        self.counts = [counts[axis] for axis in axes]
        self.me = [lax.axis_index(axis) for axis in axes]
        self.moves = other_moves(self.counts)

    def start(self, source, target=None):
        places = [
            [lax.rem(m + d, n) for d in range(n)] for m, n in zip(self.me, self.counts)
        ]
        for slot, move in enumerate(self.moves):
            other = [place[d] for place, d in zip(places, move)]
            pltpu.make_async_remote_copy(
                src_ref=source(*other),
                dst_ref=self.recv.at[slot] if target is None else target,
                send_sem=self.sems.at[0],
                recv_sem=self.sems.at[1],
                device_id=dict(zip(self.axes, other)),
                device_id_type=MESH,
            ).start()

    def wait(self):
        pltpu.make_async_copy(self.recv, self.recv, self.sems.at[1]).wait()

    def drain(self):
        pltpu.make_async_copy(self.recv, self.recv, self.sems.at[0]).wait()

    def total(self, own):
        parts = [own] + [self.recv[slot] for slot in range(len(self.moves))]
        while len(parts) > 1:
            odd = parts[len(parts) // 2 * 2 :]
            parts = [a + b for a, b in zip(parts[0::2], parts[1::2])] + odd
        return parts[0]


def other_moves(counts):
    def hops(move):
        return sum(min(d, n - d) for d, n in zip(move, counts))

    moves = [m for m in itertools.product(*(range(n) for n in counts)) if any(m)]
    return sorted(moves, key=hops, reverse=True)


class StateSum:
    def __init__(self, first, last, counts, state, r1, p1, r2, full, sems):
        self.state, self.p1, self.full = state, p1, full
        self.tile, self.nx = p1.shape[0], counts[X]
        self.scatter = Exchange((first, X), counts, r1, sems.at[0])
        self.line = Exchange((last,), counts, r2, sems.at[1])
        self.gather = Exchange((first, X), counts, r1, sems.at[2])

    def spot(self, first, x):
        return pl.ds(pl.multiple_of((first * self.nx + x) * self.tile, 8), self.tile)

    def start(self):
        self.scatter.start(lambda first, x: self.state.at[self.spot(first, x)])

    def second(self):
        self.scatter.wait()
        self.p1[...] = self.scatter.total(self.state[self.spot(*self.scatter.me)])
        self.line.start(lambda j: self.p1)

    def third(self):
        self.line.wait()
        own = self.spot(*self.scatter.me)
        self.full[own] = self.line.total(self.p1[...])
        self.gather.start(lambda first, x: self.full.at[own], self.full.at[own])

    def finish(self):
        self.gather.wait()

    def drain(self):
        for step in (self.scatter, self.line, self.gather):
            step.drain()


class RowSum:
    def __init__(self, first, last, counts, source, plane, line, result, sems):
        self.source, self.result = source, result
        self.plane = Exchange((first, X), counts, plane, sems.at[0])
        self.line = Exchange((last,), counts, line, sems.at[1])

    def start(self):
        self.plane.start(lambda *_: self.source.at[0])

    def second(self):
        self.plane.wait()
        self.source[1] = self.plane.total(self.source[0])
        self.line.start(lambda _: self.source.at[1])

    def finish(self):
        self.line.wait()
        self.result[...] = self.line.total(self.source[1])

    def drain(self):
        for step in (self.plane, self.line):
            step.drain()


class TokenRing:
    def __init__(self, counts, grads, recv, sems):
        self.grads, self.recv, self.sems = grads, recv, sems
        self.me, self.count = lax.axis_index(X), counts[X]
        half = grads.shape[0] // 2
        self.top, self.low = pl.ds(0, half), pl.ds(half, half)

    def copy(self, i, source, slot, rows, step):
        return pltpu.make_async_remote_copy(
            src_ref=source.at[rows],
            dst_ref=self.recv.at[slot, rows],
            send_sem=self.sems.at[0, i],
            recv_sem=self.sems.at[1, i],
            device_id={X: lax.rem(self.me + step, self.count)},
            device_id_type=MESH,
        )

    def copies(self):
        right, left = 1, self.count - 1
        return [
            self.copy(0, self.grads, 1, self.top, right),
            self.copy(1, self.grads, 2, self.low, left),
            self.copy(2, self.grads, 1, self.low, right),
            self.copy(3, self.grads, 2, self.top, left),
            self.copy(4, self.recv.at[1], 0, self.top, right),
            self.copy(5, self.recv.at[2], 0, self.low, left),
        ]

    def start(self):
        for copy in self.copies()[:4]:
            copy.start()

    def relay(self):
        copies = self.copies()
        for i in range(2):
            copies[i].wait_recv()
            copies[4 + i].start()

    def wait(self):
        for copy in self.copies()[2:]:
            copy.wait_recv()

    def drain(self):
        for copy in self.copies():
            copy.wait_send()


class WeightSum:
    def __init__(self, counts, hid_t, grads, rx, ring, part, r1, p1, r2, sems):
        self.hid_t, self.grads, self.part, self.p1 = hid_t, grads, part, p1
        self.x = TokenRing(counts, grads, rx, ring)
        self.count = counts[X]
        self.near = p1.shape[1]
        self.one = [
            Exchange((axis,), counts, r1.at[i], sems.at[i]) for i, axis in enumerate((Y, Z))
        ]
        self.two = [
            Exchange((axis,), counts, r2.at[i], sems.at[2 + i]) for i, axis in enumerate((Z, Y))
        ]

    def start(self):
        self.x.start()

    def second(self):
        self.x.wait()
        for i in range(2):
            side = slice(i * 128, (i + 1) * 128)
            total = None
            for s in range(self.count):
                rows = self.grads[:, side] if s == 0 else self.x.recv[s - 1, :, side]
                term = dg(self.hid_t[i, s], rows.astype(BF16), 1, 0)
                total = term if total is None else total + term
            self.part[i] = total
            self.one[i].start(
                lambda j, i=i: self.part.at[i, pl.ds(pl.multiple_of(j * self.near, 8), self.near)]
            )

    def third(self):
        for i in range(2):
            one = self.one[i]
            one.wait()
            own = self.part[i, pl.ds(pl.multiple_of(one.me[0] * self.near, 8), self.near)]
            self.p1[i] = one.total(own)
            self.two[i].start(
                lambda j, i=i: self.p1.at[i, pl.ds(pl.multiple_of(lax.div(j, 2) * 8, 8), 8)]
            )

    def finish(self, out):
        for i in range(2):
            two = self.two[i]
            two.wait()
            tile = two.total(self.p1[i, pl.ds(pl.multiple_of(lax.div(two.me[0], 2) * 8, 8), 8)])
            low = lax.rem(two.me[0], 2) == 0
            out[:, i * 128 : (i + 1) * 128] = jnp.where(low, tile[0:4], tile[4:8])

    def drain(self):
        for step in [self.x] + self.one + self.two:
            step.drain()


def interleave(upper, a, b):
    return jnp.where(upper, a, pltpu.roll(b, 4, 1)), jnp.where(upper, pltpu.roll(a, 4, 1), b)


def halves(shape):
    return lax.broadcasted_iota(jnp.int32, shape, 1) < 4


def by_x(turned, out):
    nx, rows, toks = out.shape
    tiles = turned.reshape(rows // 8, 2, nx // 2, 8, toks)
    upper = halves((rows // 8, 8, toks))
    for p in range(nx // 2):
        even, odd = interleave(upper, tiles[:, 0, p], tiles[:, 1, p])
        out[2 * p] = even.reshape(rows, toks)
        out[2 * p + 1] = odd.reshape(rows, toks)


def swapped(block, ny, nz):
    rows, toks = block.shape
    tiles = block.reshape(ny // 2, 2, nz // 2, 8, toks)
    upper = halves((ny // 2, 8, toks))
    out = []
    for w in range(nz // 2):
        out.extend(interleave(upper, tiles[:, 0, w], tiles[:, 1, w]))
    return jnp.concatenate([t.reshape(ny * 4, toks) for t in out], axis=0)


def kernel(counts, heads, dh, feat, *refs):
    inputs, (gh, gv, gq, gk), scratch = refs[:6], refs[6:10], refs[10:]
    (qs, ks, fa, fb, st, r1, p1, r2, full, st_sem) = scratch[:10]
    (zsrc, zp, zl, ztot, z_sem) = scratch[10:15]
    (grads, rx, ring_sem, wpart, w1, wp1, w2, w_sem) = scratch[15:23]
    (turned, rturned, hid_t, turned_sem) = scratch[23:27]
    (part, rpart, part_sem) = scratch[27:30]
    hid, wq, wk, val, gout, tab, in_sem = scratch[30:]
    ny, nz, nx = counts[Y], counts[Z], counts[X]
    sizes = {**counts, H: 2}
    scale = dh ** (-0.25)
    norm = feat ** (-0.5)

    barrier = pltpu.get_barrier_semaphore()
    partners = set()
    for axes in ((Y, X), (Z, X), (H,)):
        for move in other_moves([sizes[axis] for axis in axes]):
            partners.add(tuple(sorted(zip(axes, move))))
    partners = sorted({tuple((a, d) for a, d in move if d) for move in partners})
    for move in partners:
        place = {a: lax.rem(lax.axis_index(a) + d, sizes[a]) for a, d in move}
        pl.semaphore_signal(barrier, inc=1, device_id=place, device_id_type=MESH)

    loads = [
        pltpu.make_async_copy(source, target, in_sem.at[i])
        for i, (source, target) in enumerate(zip(inputs, (hid, wq, wk, val, gout, tab)))
    ]
    for i in (0, 2, 5, 3, 1, 4):
        loads[i].start()

    def state_sum(c):
        return [
            StateSum(
                (Y, Z)[i], (Z, Y)[i], counts, st.at[c, i], r1.at[c, i], p1.at[c, i], r2.at[c, i],
                full.at[c, i], st_sem.at[c, i],
            )
            for i in range(2)
        ]

    def row_sum(c):
        return [
            RowSum(
                (Y, Z)[i], (Z, Y)[i], counts, zsrc.at[c, i], zp.at[c, i], zl.at[c, i],
                ztot.at[c, i], z_sem.at[c, i],
            )
            for i in range(2)
        ]

    def weight_sum(c):
        return WeightSum(
            counts, hid_t, grads.at[c], rx.at[c], ring_sem.at[c], wpart.at[c], w1.at[c], wp1.at[c], w2.at[c], w_sem.at[c]
        )

    usum, gsum = state_sum(0), state_sum(1)
    zsum, gzsum = row_sum(0), row_sum(1)
    qsum, ksum = weight_sum(0), weight_sum(1)
    hsum = Exchange((X,), counts, rturned, turned_sem)

    def cols(h):
        return slice(h * dh, (h + 1) * dh)

    def wide(h):
        return slice(h * feat, (h + 1) * feat)

    def half_row(h):
        return h // (heads // 2), wide(h % (heads // 2))

    def total_row(c, h):
        i, spot = half_row(h)
        return ztot[c, i, :, spot]

    def put_row(c, h, row):
        i, spot = half_row(h)
        zsrc[c, i, 0, :, spot] = row

    def features(rows, h):
        own = rows[:, cols(h)]
        logits = dot3(own, tab[h])
        half = 0.5 * jnp.sum(own * own, axis=1, keepdims=True)
        return jnp.exp(logits - half) * norm

    def put_state(c, h, block):
        st[c, 0, cols(h)] = block[:, 0:128]
        st[c, 1, cols(h)] = block[:, 128:256]

    def state(c, h):
        return jnp.concatenate([full[c, 0, cols(h)], full[c, 1, cols(h)]], axis=1)

    loads[0].wait()
    loads[2].wait()
    k = dg(hid[...], wk[...], 1, 0) * scale
    ks[...] = k
    loads[3].wait()
    loads[5].wait()
    vt = val[...].astype(F32).T.astype(BF16)
    for h in range(heads):
        b = features(k, h)
        fb[:, wide(h)] = b
        put_row(0, h, jnp.sum(b, axis=0, keepdims=True))
        put_state(0, h, dot2(vt[cols(h)], b))
    pl.semaphore_wait(barrier, len(partners))
    for s in zsum:
        s.start()
    for s in usum:
        s.start()
    by_x(hid[...].astype(F32).T, turned)
    hsum.start(lambda j: turned.at[j])

    loads[1].wait()
    loads[4].wait()
    q = dg(hid[...], wq[...], 1, 0) * scale
    qs[...] = q
    for h in range(heads):
        fa[:, wide(h)] = features(q, h)
    for s in zsum:
        s.second()
    for s in usum:
        s.second()
    for s in zsum:
        s.finish()

    g = gout[...].astype(F32)
    inv, gn = [], []
    for h in range(heads):
        a = fa[:, wide(h)]
        den = jnp.sum(a * total_row(0, h), axis=1, keepdims=True)
        inv.append(1.0 / den)
        gn.append(g[:, cols(h)] / den)
    gnt = jnp.concatenate(gn, axis=1).T
    for h in range(heads):
        put_state(1, h, dot3(gnt[cols(h)], fa[:, wide(h)]))
    for s in gsum:
        s.start()
    for s in usum:
        s.third()
    hsum.wait()
    for i in range(nx):
        block = turned[hsum.me[0]] if i == 0 else rturned[i - 1]
        hid_t[0, i] = block.astype(BF16)
        hid_t[1, i] = swapped(block, ny, nz).astype(BF16)
    for s in gsum:
        s.second()
    for s in usum:
        s.finish()

    gd = []
    for h in range(heads):
        a = fa[:, wide(h)]
        o = dot3(a, state(0, h), 1, 1) * inv[h]
        gd.append(-jnp.sum(g[:, cols(h)] * o, axis=1, keepdims=True) * inv[h])
        put_row(1, h, jnp.sum(gd[h] * a, axis=0, keepdims=True))
    for s in gzsum:
        s.start()
    for s in gsum:
        s.third()

    def back(rows, h, weighted):
        got = dot3(weighted, tab[h], 1, 1)
        total = jnp.sum(weighted, axis=1, keepdims=True)
        return ((got - rows[:, cols(h)] * total) * scale).astype(BF16)

    dq = []
    for h in range(heads):
        ga = dot3(gn[h], state(0, h)) + gd[h] * total_row(0, h)
        dq.append(back(qs, h, fa[:, wide(h)] * ga))
    dq = jnp.concatenate(dq, axis=1)
    for s in gzsum:
        s.second()
    grads[0] = dq.astype(F32)
    qsum.start()
    part[...] = dg(dq, wq[...], 1, 1)
    for s in gsum:
        s.finish()
    qsum.x.relay()
    lifted = [dot2(val[:, cols(h)], state(1, h)) for h in range(heads)]
    for h in range(heads):
        gv[:, cols(h)] = dot3(fb[:, wide(h)], state(1, h), 1, 1).astype(BF16)
    for s in gzsum:
        s.finish()

    dk = []
    for h in range(heads):
        gb = lifted[h] + total_row(1, h)
        dk.append(back(ks, h, fb[:, wide(h)] * gb))
    dk = jnp.concatenate(dk, axis=1)
    grads[1] = dk.astype(F32)
    ksum.start()
    part[...] += dg(dk, wk[...], 1, 1)
    swap = pltpu.make_async_remote_copy(
        src_ref=part,
        dst_ref=rpart,
        send_sem=part_sem.at[0],
        recv_sem=part_sem.at[1],
        device_id={H: 1 - lax.axis_index(H)},
        device_id_type=MESH,
    )
    swap.start()
    ksum.x.relay()
    qsum.second()
    ksum.second()
    qsum.third()
    swap.wait_recv()
    gh[...] = part[...] + rpart[...]
    ksum.third()
    qsum.finish(gq)
    ksum.finish(gk)
    swap.wait_send()
    for s in usum + gsum + zsum + gzsum + [qsum, ksum, hsum]:
        s.drain()


def settle(*refs):
    sems = refs[8]
    copies = [
        pltpu.make_async_copy(source, target, sems.at[i])
        for i, (source, target) in enumerate(zip(refs[:4], refs[4:8]))
    ]
    for copy in copies:
        copy.start()
    for copy in copies:
        copy.wait()


def shards(counts, hidden, query_weight, key_weight, values, grad_out, random_feats):
    toks, depth = hidden.shape
    inputs = (hidden, query_weight, key_weight, values, grad_out, random_feats)
    inputs = [pltpu.with_memory_space_constraint(a, pltpu.HBM) for a in inputs]
    heads, dh, feat = random_feats.shape
    width = heads * dh
    ny, nz, nx = counts[Y], counts[Z], counts[X]
    tile = width // (ny * nx)
    own_rows = depth // (ny * nz * nx)
    row = heads * feat
    rows = depth // nx
    vm = lambda *shape: pltpu.VMEM(shape, F32)
    dma = lambda *shape: pltpu.SemaphoreType.DMA(shape)
    scratch = [
        vm(toks, width),
        vm(toks, width),
        vm(toks, row),
        vm(toks, row),
        vm(2, 2, width, 128),
        vm(2, 2, ny * nx - 1, tile, 128),
        vm(2, 2, tile, 128),
        vm(2, 2, nz - 1, tile, 128),
        vm(2, 2, width, 128),
        dma(2, 2, 3, 2),
        vm(2, 2, 2, 1, row // 2),
        vm(2, 2, ny * nx - 1, 1, row // 2),
        vm(2, 2, nz - 1, 1, row // 2),
        vm(2, 2, 1, row // 2),
        dma(2, 2, 2, 2),
        vm(2, toks, width),
        vm(2, nx - 1, toks, width),
        dma(2, 2, 6),
        vm(2, 2, rows, 128),
        vm(2, 2, ny - 1, rows // ny, 128),
        vm(2, 2, rows // ny, 128),
        vm(2, 2, nz - 1, 8, 128),
        dma(2, 4, 2),
        vm(nx, rows, toks),
        vm(nx - 1, rows, toks),
        pltpu.VMEM((2, nx, rows, toks), BF16),
        dma(2),
        vm(toks, depth),
        vm(toks, depth),
        dma(2),
        *(pltpu.VMEM(a.shape, a.dtype) for a in inputs),
        dma(6),
    ]
    shapes = (
        jax.ShapeDtypeStruct((toks, depth), F32),
        jax.ShapeDtypeStruct((toks, width), BF16),
        jax.ShapeDtypeStruct((own_rows, width), F32),
        jax.ShapeDtypeStruct((own_rows, width), F32),
    )
    vmem = pl.BlockSpec(memory_space=pltpu.VMEM)
    results = pl.pallas_call(
        functools.partial(kernel, counts, heads, dh, feat),
        out_shape=shapes,
        in_specs=[pl.BlockSpec(memory_space=pltpu.HBM)] * 6,
        out_specs=(vmem,) * 4,
        scratch_shapes=scratch,
        compiler_params=pltpu.CompilerParams(
            collective_id=0, has_side_effects=True, vmem_limit_bytes=28 * 2**20
        ),
        name="favor_backward",
    )(*inputs)
    return pl.pallas_call(
        settle,
        out_shape=shapes,
        in_specs=[vmem] * 4,
        out_specs=(pl.BlockSpec(memory_space=pl.ANY),) * 4,
        scratch_shapes=[pltpu.SemaphoreType.DMA((4,))],
        compiler_params=pltpu.CompilerParams(vmem_limit_bytes=8 * 2**20),
        name="settle",
    )(*results)


def build(torus):
    counts = {axis: torus.shape[axis] for axis in SEQ}
    return jax.shard_map(
        functools.partial(shards, counts),
        mesh=torus,
        in_specs=(
            P(SEQ, None),
            P(None, H),
            P(None, H),
            P(SEQ, H),
            P(SEQ, H),
            P(H, None, None),
        ),
        out_specs=(P(SEQ, None), P(SEQ, H), P(SEQ, H), P(SEQ, H)),
        check_vma=False,
    )


def solution(mesh):
    devices = mesh.devices.reshape(8, 8, 4, mesh.shape["head"])
    return build(Mesh(devices, (Y, Z, X, H)))
```
